32 devices in a mesh: aa: 2 (over y), ba: 4 (over x, core), col: 4 (over z).
Axes of the slice: x: 2, y: 2, z: 4, core: 2. Of those that a mesh axis runs over, the one named last changes fastest.
Arguments:
- hidden: bfloat16 [2, 4, 32, 8192], P('aa', 'ba', None, 'col'), may hold values from -36 to 60, as said below
- unembed: bfloat16 [8192, 152064], P(None, ('aa', 'ba', 'col')), may hold values from -1 to 5, as said below
- targets: int32 [2, 4, 32], replicated, may hold values from 0 to 152063
- lengths: int32 [2, 4], replicated, may hold values from 1 to 32
Outputs:
- scores: float32 [2, 4], P('aa', 'ba')
The draws below stay inside these ranges and needn't reach their ends.
Inputs may be any that keep to these rules, and one draw needn't show every extreme that they name: real-valued hidden states. `unembed`: real-valued unembedding entries.
All inputs are finite; a program needn't handle non-finite values.
Results may differ from the reference program's by a relative error of at most 0.0003.
Values may be sent and summed in bfloat16 or wider, within the bound.
A program may use at most 128 MiB of HBM per device.

```python
import jax
import jax.numpy as jnp

D = 8192
VOCAB = 152064
CHOICES = 4
LEN = 32
QUEST = 2


def draw_unembed(key, part):
    base = jax.random.truncated_normal(key, -6.0, 6.0, (D, VOCAB), jnp.float32) * D ** (-0.5)
    return base.astype(jnp.bfloat16)


def draw_hidden(key, part):
    shape = (QUEST, CHOICES, LEN, D)
    base = 3.0 * jax.random.truncated_normal(key, -8.0, 8.0, shape, jnp.float32)
    return base.astype(jnp.bfloat16)


def with_ends(result, own_key, low, top_value):
    longest = result.shape.index(max(result.shape))
    spots = []
    for shift in (0, 1):
        where = [jax.random.randint(jax.random.fold_in(own_key, axis), (), 0, length) for axis, length in enumerate(result.shape)]
        where[longest] = (where[longest] + shift) % result.shape[longest]
        spots.append(tuple(where))
    return result.at[spots[0]].set(low).at[spots[1]].set(top_value)


def setup_inputs(seed: int = 0) -> dict:
    key_list = jax.random.split(jax.random.key(seed), 5)
    hidden = draw_hidden(jax.random.fold_in(key_list[4], 71), 0)
    unembed = draw_unembed(jax.random.fold_in(key_list[4], 71), 0)
    targets = with_ends(jax.random.randint(key_list[2], (QUEST, CHOICES, LEN), 0, VOCAB), jax.random.fold_in(key_list[2], 1), 0, VOCAB - 1).astype(jnp.int32)
    lengths = with_ends(jax.random.randint(key_list[3], (QUEST, CHOICES), 1, LEN + 1), jax.random.fold_in(key_list[3], 1), 1, LEN).astype(jnp.int32)
    return dict(hidden=hidden, unembed=unembed, targets=targets, lengths=lengths)


def reference(hidden, unembed, targets, lengths):
    rows = hidden.reshape(-1, D)
    logits = jnp.dot(rows, unembed, preferred_element_type=jnp.float32)
    top = jnp.max(logits, axis=1)
    total = jnp.sum(jnp.exp(logits - top[:, None]), axis=1)
    picked = jnp.take_along_axis(logits, targets.reshape(-1, 1).astype(jnp.int32), axis=1)[:, 0]
    logprob = (picked - top - jnp.log(total)).reshape(QUEST, CHOICES, LEN)
    positions = jnp.arange(LEN, dtype=jnp.int32)
    valid = positions[None, None, :] < lengths[:, :, None]
    summed = jnp.sum(jnp.where(valid, logprob, jnp.zeros_like(logprob)), axis=2)
    return summed / lengths.astype(jnp.float32)
```

```python
import functools
import math

import jax
import jax.numpy as jnp
from jax import lax
from jax.experimental import pallas as pl
from jax.experimental.pallas import tpu as pltpu
from jax.sharding import PartitionSpec as P

MESH = pl.DeviceIdType.MESH
LINK = 0.7
LATENCY = 1.8
COLUMN = 2.3
MATE = 1.1
SHADOW = 1.5
SLACK = 0.8
SINGLE = 1.62
PAIR = 2.95
WEIGHT = 1.42
SINGLES = 6
FLIGHT = 4
VMEM_BUDGET = 59 * 2**20
Z, X, A, DIAG, SIB = range(5)


def round_up(value, to):
    return (value + to - 1) // to * to


def flip(value, step, count):
    if count & (count - 1):
        return lax.rem(value + step, count)
    bit = 1
    while bit < count:
        on = lax.rem(step // bit, 2)
        value = value + on * (bit - 2 * bit * lax.rem(value // bit, 2))
        bit *= 2
    return value


def schedule(chunks, n_c, slots, quanta):
    units = n_c * chunks
    ready = {(0, i): 0.0 for i in range(chunks)}
    clock = COLUMN
    for i in range(chunks, units):
        clock += LINK * min(2, i // chunks)
        ready[0, i] = clock
    lists, now, busy, first, fed = [], 0.0, 0.0, 0, min(FLIGHT, slots)
    for q, count in enumerate(quanta):
        out = []
        here = [(2, i) for i in range(first, first + count)]
        soon = [(2, i) for i in range(first + count, first + count + quanta[min(q + 1, len(quanta) - 1)])]
        waited = False
        while ready:
            key = min(ready, key=lambda key: (ready[key], -key[0], key[1]))
            must = any(kind < 2 and (2, i) in here or (kind, i) in here for kind, i in ready)
            ahead = any((kind, i) in soon and at < now + SLACK for (kind, i), at in ready.items())
            if ready[key] > now and not must and not (q and ahead):
                if waited:
                    now += MATE if q else SHADOW
                    waited = False
                    continue
                break
            if ready[key] > now:
                waited = waited or must
                now = ready[key]
            kind, i = key
            del ready[key]
            out.append(key)
            if kind < 2:
                busy = max(now, busy) + LINK / (1 + kind)
                ready[kind + 1, i] = busy + LATENCY
            limit = first + slots if q else min(slots, FLIGHT + int((now + 2.0) / WEIGHT))
            while fed < min(units, limit):
                out.append((3, fed))
                fed += 1
        while q and fed < min(units, first + slots):
            out.append((3, fed))
            fed += 1
        lists.append(out)
        first += count
        now += SINGLE if count == 1 else PAIR
    return lists


def split(units):
    single = min(SINGLES, units)
    single += (units - single) % 2
    return [1] * single + [2] * ((units - single) // 2)


def wrap(value, count):
    return jnp.where(value >= count, value - count, value)


def kernel(dims, hid_ref, w_ref, tgt_ref, len_ref, out_ref, hid, wbuf, acc, stat_send, stat_recv,
           own_sem, w_sem, recv_sem, plane_sem, z_sem, stat_send_sem, stat_recv_sem):
    n_a, n_b, n_c, rows, width, vocab, tile, slots = dims
    n_x = n_b // 2
    groups = n_a * n_b
    n_dev = groups * n_c
    chunks = hid_ref.shape[1] // width
    units = n_c * chunks
    a, b, c = lax.axis_index("aa"), lax.axis_index("ba"), lax.axis_index("col")
    x, k = b // 2, lax.rem(b, 2)
    rank = a * n_b + b
    me = rank * n_c + c
    flight = min(FLIGHT, slots)
    others_a = [wrap(a + d, n_a) for d in range(1, n_a)]
    others_x = [wrap(x + d, n_x) for d in range(1, n_x)]
    columns = [c] + [flip(c, step, n_c) for step in range(1, n_c)]

    def unit_of(i):
        if isinstance(i, int):
            return columns[i // chunks] * chunks + i % chunks
        return flip(c, i // chunks, n_c) * chunks + lax.rem(i, chunks)

    def block(u, r, count=1):
        return hid.at[u, pl.ds(pl.multiple_of(r * rows, rows), rows * count), :]

    def weights(i):
        start = pl.multiple_of(unit_of(i) * width, width)
        slot = lax.rem(i, slots)
        return pltpu.make_async_copy(w_ref.at[:, pl.ds(start, width)], wbuf.at[slot], w_sem.at[slot])

    def own(j):
        return pltpu.make_async_copy(
            hid_ref.at[:, pl.ds(j * width, width)], block(c * chunks + j, rank), own_sem.at[j])

    def send(u, r, kind, device, sem):
        pltpu.make_async_remote_copy(
            src_ref=block(u, r), dst_ref=block(u, r), send_sem=sem, recv_sem=recv_sem.at[kind, u],
            device_id=device, device_id_type=MESH).start()

    def await_blocks(u, kind, count):
        if count:
            ref = block(u, 0, count)
            pltpu.make_async_copy(ref, ref, recv_sem.at[kind, u]).wait()

    def to_sibling(u, r):
        send(u, r, SIB, (a, b + 1 - 2 * k, c), plane_sem.at[u])

    def share(u):
        for ox in others_x:
            send(u, rank, X, (a, ox * 2 + k, c), plane_sem.at[u])
        for oa in others_a:
            send(u, rank, A, (oa, b, c), plane_sem.at[u])
        to_sibling(u, rank)

    def stage0(i):
        u = unit_of(i)
        if i >= chunks:
            await_blocks(u, Z, 1)
        share(u)

    def stage1(i):
        u = unit_of(i)
        await_blocks(u, X, n_x - 1)
        await_blocks(u, A, n_a - 1)
        for oa in others_a:
            for ox in others_x:
                src = (a + (oa - a) * (1 - k)) * n_b + (x + (ox - x) * k) * 2 + k
                send(u, src, DIAG, (a + (oa - a) * k, (x + (ox - x) * (1 - k)) * 2 + k, c), plane_sem.at[u])
        for ox in others_x:
            to_sibling(u, a * n_b + ox * 2 + k)
        for oa in others_a:
            to_sibling(u, oa * n_b + b)

    def stage2(i):
        u = unit_of(i)
        await_blocks(u, DIAG, (n_a - 1) * (n_x - 1))
        for oa in others_a:
            for ox in others_x:
                to_sibling(u, oa * n_b + ox * 2 + k)

    barrier = pltpu.get_barrier_semaphore()
    partners = [(a, b + 1 - 2 * k, c)]
    partners += [(a, ox * 2 + k, c) for ox in others_x]
    partners += [(oa, b, c) for oa in others_a]
    partners += [(a, b, oc) for oc in columns[1:]]
    for device in partners:
        pl.semaphore_signal(barrier, inc=1, device_id=device, device_id_type=MESH)
    for j in range(chunks):
        own(j).start()
    acc[...] = jnp.zeros_like(acc)
    stat_send[...] = jnp.zeros_like(stat_send)
    for j in range(chunks):
        own(j).wait()
    for i in range(flight):
        weights(i).start()
    pl.semaphore_wait(barrier, len(partners))

    def to_column(step, j):
        send(c * chunks + j, rank, Z, (a, b, columns[step]), z_sem.at[j])

    actions = (stage0, stage1, stage2, lambda i: weights(i).start())
    quanta = split(units)
    plan = schedule(chunks, n_c, slots, quanta)

    def run(steps):
        for kind, i in steps:
            actions[kind](i)

    own_steps, rest = plan[0][:chunks], plan[0][chunks:]
    for j, (kind, i) in enumerate(own_steps):
        actions[kind](i)
        if n_c > 1:
            to_column(1, j)
    for step in range(2, n_c):
        for j in range(chunks):
            to_column(step, j)
    run(rest)

    def product(first, count, span):
        total = acc[span, :]
        for i in range(count):
            total += lax.dot_general(
                wbuf[lax.rem(first + i, slots), span, :], hid[unit_of(first + i)], (((1,), (1,)), ((), ())),
                preferred_element_type=jnp.float32)
        return total

    def arrive(first, count):
        for i in range(count):
            weights(first + i).wait()
        for i in range(count):
            await_blocks(unit_of(first + i), SIB, groups // 2)

    spans = [pl.ds(n, min(tile, vocab - n)) for n in range(0, vocab, tile)]
    begin = 0
    for count in (1, 2):
        start = sum(quanta[:begin])
        number = quanta.count(count) - (count == quanta[-1])

        @pl.loop(0, number)
        def _(t, count=count, start=start, begin=begin, number=number):
            for q in range(number):
                if begin + q and plan[begin + q]:
                    pl.when(t == q)(lambda q=q: run(plan[begin + q]))
            first = start + t * count
            arrive(first, count)
            for span in spans:
                acc[span, :] = product(first, count, span)

        begin += number

    run(plan[begin])
    count = quanta[-1]
    arrive(units - count, count)
    ids = jnp.concatenate(
        [tgt_ref[g // n_b, g % n_b:g % n_b + 1, :] for g in range(groups)], axis=1) - me * vocab
    tops, totals, picks = [], [], []
    for span in spans:
        acc[span, :] = product(units - count, count, span)
        part = acc[span, :]
        top = jnp.max(part, axis=0, keepdims=True)
        at = lax.broadcasted_iota(jnp.int32, part.shape, 0) + span.start
        tops.append(top)
        totals.append(jnp.sum(jnp.exp(part - top), axis=0, keepdims=True))
        picks.append(jnp.sum(jnp.where(at == ids, part, 0.0), axis=0, keepdims=True))
    top = functools.reduce(jnp.maximum, tops)
    total = sum(s * jnp.exp(m - top) for s, m in zip(totals, tops))
    picked = sum(picks)
    for t in range(groups * rows // 128):
        lanes = slice(t * 128, (t + 1) * 128)
        stat_send[t, 0:1, :] = top[:, lanes]
        stat_send[t, 1:2, :] = total[:, lanes]
        stat_send[t, 2:3, :] = picked[:, lanes]

    all_a, all_b = [a] + others_a, [b] + [wrap(b + d, n_b) for d in range(1, n_b)]
    for oa in reversed(all_a):
        for ob in reversed(all_b):
            for oc in reversed(columns):
                if oa is a and ob is b and oc is c:
                    continue
                pltpu.make_async_remote_copy(
                    src_ref=stat_send.at[(oa * n_b + ob) * rows // 128], dst_ref=stat_recv.at[me],
                    send_sem=stat_send_sem, recv_sem=stat_recv_sem, device_id=(oa, ob, oc),
                    device_id_type=MESH).start()

    stat_recv[me] = stat_send[rank * rows // 128]

    for u in range(units):
        ref = block(u, 0, groups - 1)
        pltpu.make_async_copy(ref, ref, plane_sem.at[u]).wait()
    if n_c > 1:
        for j in range(chunks):
            ref = hid.at[pl.ds(0, n_c - 1), 0:rows, :]
            pltpu.make_async_copy(ref, ref, z_sem.at[j]).wait()

    ref = stat_recv.at[pl.ds(0, n_dev - 1)]
    pltpu.make_async_copy(ref, ref, stat_recv_sem).wait()
    tops = stat_recv[:, 0:1, :]
    top = jnp.max(tops, axis=0, keepdims=True)
    total = jnp.sum(stat_recv[:, 1:2, :] * jnp.exp(tops - top), axis=0)
    picked = jnp.sum(stat_recv[:, 2:3, :], axis=0)
    logprob = picked - top[0] - jnp.log(total)
    live = len_ref[a, b]
    position = lax.broadcasted_iota(jnp.int32, logprob.shape, 1) - lax.rem(rank * rows, 128)
    valid = jnp.logical_and(position >= 0, position < live)
    summed = jnp.sum(jnp.where(valid, logprob, 0.0), axis=1, keepdims=True)
    out_ref[...] = summed / jnp.full((1, 1), live, jnp.int32).astype(jnp.float32)
    ref = stat_recv.at[pl.ds(0, n_dev - 1)]
    pltpu.make_async_copy(ref, ref, stat_send_sem).wait()


def body(hidden, unembed, targets, lengths):
    n_a, n_b, n_c = (lax.axis_size(name) for name in ("aa", "ba", "col"))
    rows = hidden.shape[0] * hidden.shape[1] * hidden.shape[2]
    part = hidden.shape[3]
    vocab = unembed.shape[1]
    width = math.gcd(part, 512)
    chunks = part // width
    units = n_c * chunks
    groups = n_a * n_b
    n_dev = groups * n_c
    padded = round_up(vocab, 8)
    tile = max(t for t in range(8, min(vocab, 800) + 1, 8) if vocab % 8 or vocab % t == 0)
    held = groups * rows * (units * width * 2 + padded * 4) + (n_dev + groups) * 4096
    slots = min(units, (VMEM_BUDGET - held) // (width * padded * 2))
    dims = (n_a, n_b, n_c, rows, width, vocab, tile, slots)
    return pl.pallas_call(
        functools.partial(kernel, dims),
        out_shape=jax.ShapeDtypeStruct((1, 1), jnp.float32),
        in_specs=[
            pl.BlockSpec(memory_space=pl.ANY),
            pl.BlockSpec(memory_space=pl.ANY),
            pl.BlockSpec(memory_space=pltpu.VMEM),
            pl.BlockSpec(memory_space=pltpu.SMEM),
        ],
        out_specs=pl.BlockSpec(memory_space=pltpu.VMEM),
        scratch_shapes=[
            pltpu.VMEM((units, groups * rows, width), jnp.bfloat16),
            pltpu.VMEM((slots, vocab, width), jnp.bfloat16),
            pltpu.VMEM((vocab, groups * rows), jnp.float32),
            pltpu.VMEM((groups * rows // 128, 8, 128), jnp.float32),
            pltpu.VMEM((n_dev, 8, 128), jnp.float32),
            pltpu.SemaphoreType.DMA((chunks,)),
            pltpu.SemaphoreType.DMA((slots,)),
            pltpu.SemaphoreType.DMA((5, units)),
            pltpu.SemaphoreType.DMA((units,)),
            pltpu.SemaphoreType.DMA((chunks,)),
            pltpu.SemaphoreType.DMA,
            pltpu.SemaphoreType.DMA,
        ],
        compiler_params=pltpu.CompilerParams(
            collective_id=0, has_side_effects=True, vmem_limit_bytes=67_043_328),
    )(hidden.reshape(rows, part), unembed.T, targets, lengths)


def solution(mesh):
    in_specs = (P("aa", "ba", None, "col"), P(None, ("aa", "ba", "col")), P(), P())
    out_specs = P("aa", "ba")
    return jax.shard_map(body, mesh=mesh, in_specs=in_specs, out_specs=out_specs, check_vma=False)
```

```python
import functools
import math

import jax
import jax.numpy as jnp
from jax import lax
from jax.experimental import pallas as pl
from jax.experimental.pallas import tpu as pltpu
from jax.sharding import PartitionSpec as P

MESH = pl.DeviceIdType.MESH
LINK = 0.7
LATENCY = 1.6
COLUMN = 2.3
MATE = 1.1
SHADOW = 1.5
SLACK = 0.8
SINGLE = 1.62
PAIR = 2.95
WEIGHT = 1.42
SINGLES = 6
FLIGHT = 4
DIRECT = 1
HOP = 0.5
VMEM_BUDGET = 59 * 2**20
Z, X, A, DIAG, SIB = range(5)


def round_up(value, to):
    return (value + to - 1) // to * to


def flip(value, step, count):
    if count & (count - 1):
        return lax.rem(value + step, count)
    bit = 1
    while bit < count:
        on = lax.rem(step // bit, 2)
        value = value + on * (bit - 2 * bit * lax.rem(value // bit, 2))
        bit *= 2
    return value


def schedule(chunks, n_c, slots, quanta):
    units = n_c * chunks
    ready = {(0, i): 0.0 for i in range(chunks)}
    clock = COLUMN
    for i in range(chunks, units):
        clock += LINK * min(2, i // chunks)
        ready[0, i] = clock
    lists, now, busy, first, fed = [], 0.0, 0.0, 0, min(FLIGHT, slots)
    for q, count in enumerate(quanta):
        out = []
        here = [(2, i) for i in range(first, first + count)]
        soon = [(2, i) for i in range(first + count, first + count + quanta[min(q + 1, len(quanta) - 1)])]
        waited = False
        while ready:
            key = min(ready, key=lambda key: (ready[key], -key[0], key[1]))
            must = any(kind < 2 and (2, i) in here or (kind, i) in here for kind, i in ready)
            ahead = any((kind, i) in soon and at < now + SLACK for (kind, i), at in ready.items())
            if ready[key] > now and not must and not (q and ahead):
                if waited:
                    now += MATE if q else SHADOW
                    waited = False
                    continue
                break
            if ready[key] > now:
                waited = waited or must
                now = ready[key]
            kind, i = key
            del ready[key]
            out.append(key)
            if kind < 2:
                busy = max(now, busy) + LINK / (1 + kind)
                if i < DIRECT and kind == 0:
                    busy += LINK
                    ready[2, i] = busy + LATENCY + HOP
                if i >= DIRECT or kind == 0:
                    ready[kind + 1, i] = busy + LATENCY
            limit = first + slots if q else min(slots, FLIGHT + int((now + 2.0) / WEIGHT))
            while fed < min(units, limit):
                out.append((3, fed))
                fed += 1
        while q and fed < min(units, first + slots):
            out.append((3, fed))
            fed += 1
        lists.append(out)
        first += count
        now += SINGLE if count == 1 else PAIR
    return lists


def split(units):
    single = min(SINGLES, units)
    single += (units - single) % 2
    return [1] * single + [2] * ((units - single) // 2)


def wrap(value, count):
    return jnp.where(value >= count, value - count, value)


def kernel(dims, hid_ref, w_ref, tgt_ref, len_ref, out_ref, hid, wbuf, acc, stat_send, stat_recv,
           own_sem, w_sem, recv_sem, plane_sem, z_sem, stat_send_sem, stat_recv_sem):
    n_a, n_b, n_c, rows, width, vocab, tile, slots = dims
    n_x = n_b // 2
    groups = n_a * n_b
    n_dev = groups * n_c
    chunks = hid_ref.shape[1] // width
    units = n_c * chunks
    a, b, c = lax.axis_index("aa"), lax.axis_index("ba"), lax.axis_index("col")
    x, k = b // 2, lax.rem(b, 2)
    rank = a * n_b + b
    me = rank * n_c + c
    flight = min(FLIGHT, slots)
    others_a = [wrap(a + d, n_a) for d in range(1, n_a)]
    others_x = [wrap(x + d, n_x) for d in range(1, n_x)]
    columns = [c] + [flip(c, step, n_c) for step in range(1, n_c)]

    def unit_of(i):
        if isinstance(i, int):
            return columns[i // chunks] * chunks + i % chunks
        return flip(c, i // chunks, n_c) * chunks + lax.rem(i, chunks)

    def block(u, r, count=1):
        return hid.at[u, pl.ds(pl.multiple_of(r * rows, rows), rows * count), :]

    def weights(i):
        start = pl.multiple_of(unit_of(i) * width, width)
        slot = lax.rem(i, slots)
        return pltpu.make_async_copy(w_ref.at[:, pl.ds(start, width)], wbuf.at[slot], w_sem.at[slot])

    def own(j):
        return pltpu.make_async_copy(
            hid_ref.at[:, pl.ds(j * width, width)], block(c * chunks + j, rank), own_sem.at[j])

    def send(u, r, kind, device, sem):
        pltpu.make_async_remote_copy(
            src_ref=block(u, r), dst_ref=block(u, r), send_sem=sem, recv_sem=recv_sem.at[kind, u],
            device_id=device, device_id_type=MESH).start()

    def await_blocks(u, kind, count):
        if count:
            ref = block(u, 0, count)
            pltpu.make_async_copy(ref, ref, recv_sem.at[kind, u]).wait()

    def to_sibling(u, r):
        send(u, r, SIB, (a, b + 1 - 2 * k, c), plane_sem.at[u])

    def share(u):
        for ox in others_x:
            send(u, rank, X, (a, ox * 2 + k, c), plane_sem.at[u])
        for oa in others_a:
            send(u, rank, A, (oa, b, c), plane_sem.at[u])
        to_sibling(u, rank)

    def across(u):
        for oa in others_a:
            for ox in others_x:
                send(u, rank, DIAG, (oa, ox * 2 + k, c), plane_sem.at[u])

    def stage0(i):
        u = unit_of(i)
        if i >= chunks:
            await_blocks(u, Z, 1)
        share(u)
        if i < DIRECT:
            across(u)

    def stage1(i):
        u = unit_of(i)
        await_blocks(u, X, n_x - 1)
        await_blocks(u, A, n_a - 1)
        for oa in others_a if i >= DIRECT else []:
            for ox in others_x:
                src = (a + (oa - a) * (1 - k)) * n_b + (x + (ox - x) * k) * 2 + k
                send(u, src, DIAG, (a + (oa - a) * k, (x + (ox - x) * (1 - k)) * 2 + k, c), plane_sem.at[u])
        for ox in others_x:
            to_sibling(u, a * n_b + ox * 2 + k)
        for oa in others_a:
            to_sibling(u, oa * n_b + b)

    def stage2(i):
        u = unit_of(i)
        await_blocks(u, DIAG, (n_a - 1) * (n_x - 1))
        for oa in others_a:
            for ox in others_x:
                to_sibling(u, oa * n_b + ox * 2 + k)

    barrier = pltpu.get_barrier_semaphore()
    partners = [(a, b + 1 - 2 * k, c)]
    partners += [(a, ox * 2 + k, c) for ox in others_x]
    partners += [(oa, b, c) for oa in others_a]
    partners += [(oa, ox * 2 + k, c) for oa in others_a for ox in others_x]
    partners += [(a, b, oc) for oc in columns[1:]]
    for device in partners:
        pl.semaphore_signal(barrier, inc=1, device_id=device, device_id_type=MESH)
    for j in range(chunks):
        own(j).start()
    acc[...] = jnp.zeros_like(acc)
    stat_send[...] = jnp.zeros_like(stat_send)
    for j in range(chunks):
        own(j).wait()
    for i in range(flight):
        weights(i).start()
    pl.semaphore_wait(barrier, len(partners))

    def to_column(step, j):
        send(c * chunks + j, rank, Z, (a, b, columns[step]), z_sem.at[j])

    actions = (stage0, stage1, stage2, lambda i: weights(i).start())
    quanta = split(units)
    plan = schedule(chunks, n_c, slots, quanta)

    def run(steps):
        for kind, i in steps:
            actions[kind](i)

    own_steps, rest = plan[0][:chunks], plan[0][chunks:]
    for j, (kind, i) in enumerate(own_steps):
        actions[kind](i)
        if n_c > 1:
            to_column(1, j)
    for step in range(2, n_c):
        for j in range(chunks):
            to_column(step, j)
    run(rest)

    def product(first, count, span):
        total = acc[span, :]
        for i in range(count):
            total += lax.dot_general(
                wbuf[lax.rem(first + i, slots), span, :], hid[unit_of(first + i)], (((1,), (1,)), ((), ())),
                preferred_element_type=jnp.float32)
        return total

    def arrive(first, count):
        for i in range(count):
            weights(first + i).wait()
        for i in range(count):
            await_blocks(unit_of(first + i), SIB, groups // 2)

    spans = [pl.ds(n, min(tile, vocab - n)) for n in range(0, vocab, tile)]
    begin = 0
    for count in (1, 2):
        start = sum(quanta[:begin])
        number = quanta.count(count) - (count == quanta[-1])

        @pl.loop(0, number)
        def _(t, count=count, start=start, begin=begin, number=number):
            for q in range(number):
                if begin + q and plan[begin + q]:
                    pl.when(t == q)(lambda q=q: run(plan[begin + q]))
            first = start + t * count
            arrive(first, count)
            for span in spans:
                acc[span, :] = product(first, count, span)

        begin += number

    run(plan[begin])
    count = quanta[-1]
    arrive(units - count, count)
    ids = jnp.concatenate(
        [tgt_ref[g // n_b, g % n_b:g % n_b + 1, :] for g in range(groups)], axis=1) - me * vocab
    tops, totals, picks = [], [], []
    for span in spans:
        acc[span, :] = product(units - count, count, span)
        part = acc[span, :]
        top = jnp.max(part, axis=0, keepdims=True)
        at = lax.broadcasted_iota(jnp.int32, part.shape, 0) + span.start
        tops.append(top)
        totals.append(jnp.sum(jnp.exp(part - top), axis=0, keepdims=True))
        picks.append(jnp.sum(jnp.where(at == ids, part, 0.0), axis=0, keepdims=True))
    top = functools.reduce(jnp.maximum, tops)
    total = sum(s * jnp.exp(m - top) for s, m in zip(totals, tops))
    picked = sum(picks)
    for t in range(groups * rows // 128):
        lanes = slice(t * 128, (t + 1) * 128)
        stat_send[t, 0:1, :] = top[:, lanes]
        stat_send[t, 1:2, :] = total[:, lanes]
        stat_send[t, 2:3, :] = picked[:, lanes]

    all_a, all_b = [a] + others_a, [b] + [wrap(b + d, n_b) for d in range(1, n_b)]
    for oa in reversed(all_a):
        for ob in reversed(all_b):
            for oc in reversed(columns):
                if oa is a and ob is b and oc is c:
                    continue
                pltpu.make_async_remote_copy(
                    src_ref=stat_send.at[(oa * n_b + ob) * rows // 128], dst_ref=stat_recv.at[me],
                    send_sem=stat_send_sem, recv_sem=stat_recv_sem, device_id=(oa, ob, oc),
                    device_id_type=MESH).start()

    stat_recv[me] = stat_send[rank * rows // 128]

    for u in range(units):
        ref = block(u, 0, groups - 1)
        pltpu.make_async_copy(ref, ref, plane_sem.at[u]).wait()
    if n_c > 1:
        for j in range(chunks):
            ref = hid.at[pl.ds(0, n_c - 1), 0:rows, :]
            pltpu.make_async_copy(ref, ref, z_sem.at[j]).wait()

    ref = stat_recv.at[pl.ds(0, n_dev - 1)]
    pltpu.make_async_copy(ref, ref, stat_recv_sem).wait()
    tops = stat_recv[:, 0:1, :]
    top = jnp.max(tops, axis=0, keepdims=True)
    total = jnp.sum(stat_recv[:, 1:2, :] * jnp.exp(tops - top), axis=0)
    picked = jnp.sum(stat_recv[:, 2:3, :], axis=0)
    logprob = picked - top[0] - jnp.log(total)
    live = len_ref[a, b]
    position = lax.broadcasted_iota(jnp.int32, logprob.shape, 1) - lax.rem(rank * rows, 128)
    valid = jnp.logical_and(position >= 0, position < live)
    summed = jnp.sum(jnp.where(valid, logprob, 0.0), axis=1, keepdims=True)
    out_ref[...] = summed / jnp.full((1, 1), live, jnp.int32).astype(jnp.float32)
    ref = stat_recv.at[pl.ds(0, n_dev - 1)]
    pltpu.make_async_copy(ref, ref, stat_send_sem).wait()


def body(hidden, unembed, targets, lengths):
    n_a, n_b, n_c = (lax.axis_size(name) for name in ("aa", "ba", "col"))
    rows = hidden.shape[0] * hidden.shape[1] * hidden.shape[2]
    part = hidden.shape[3]
    vocab = unembed.shape[1]
    width = math.gcd(part, 512)
    chunks = part // width
    units = n_c * chunks
    groups = n_a * n_b
    n_dev = groups * n_c
    padded = round_up(vocab, 8)
    tile = max(t for t in range(8, min(vocab, 528) + 1, 8) if vocab % 8 or vocab % t == 0)
    held = groups * rows * (units * width * 2 + padded * 4) + (n_dev + groups) * 4096
    slots = min(units, (VMEM_BUDGET - held) // (width * padded * 2))
    dims = (n_a, n_b, n_c, rows, width, vocab, tile, slots)
    return pl.pallas_call(
        functools.partial(kernel, dims),
        out_shape=jax.ShapeDtypeStruct((1, 1), jnp.float32),
        in_specs=[
            pl.BlockSpec(memory_space=pl.ANY),
            pl.BlockSpec(memory_space=pl.ANY),
            pl.BlockSpec(memory_space=pltpu.VMEM),
            pl.BlockSpec(memory_space=pltpu.SMEM),
        ],
        out_specs=pl.BlockSpec(memory_space=pltpu.VMEM),
        scratch_shapes=[
            pltpu.VMEM((units, groups * rows, width), jnp.bfloat16),
            pltpu.VMEM((slots, vocab, width), jnp.bfloat16),
            pltpu.VMEM((vocab, groups * rows), jnp.float32),
            pltpu.VMEM((groups * rows // 128, 8, 128), jnp.float32),
            pltpu.VMEM((n_dev, 8, 128), jnp.float32),
            pltpu.SemaphoreType.DMA((chunks,)),
            pltpu.SemaphoreType.DMA((slots,)),
            pltpu.SemaphoreType.DMA((5, units)),
            pltpu.SemaphoreType.DMA((units,)),
            pltpu.SemaphoreType.DMA((chunks,)),
            pltpu.SemaphoreType.DMA,
            pltpu.SemaphoreType.DMA,
        ],
        compiler_params=pltpu.CompilerParams(
            collective_id=0, has_side_effects=True, vmem_limit_bytes=67_043_328),
    )(hidden.reshape(rows, part), unembed.T, targets, lengths)


def solution(mesh):
    in_specs = (P("aa", "ba", None, "col"), P(None, ("aa", "ba", "col")), P(), P())
    out_specs = P("aa", "ba")
    return jax.shard_map(body, mesh=mesh, in_specs=in_specs, out_specs=out_specs, check_vma=False)
```
